32 devices in a mesh: gx: 16 (over z, y, x), gy: 2 (over core).
Axes of the slice: x: 2, y: 2, z: 4, core: 2. Of those that a mesh axis runs over, the one named last changes fastest.
Arguments:
- history: bfloat16 [128, 2048, 256], P(('gx', 'gy')), may hold values from -100 to 100
- lengths: int32 [128], P(('gx', 'gy')), may hold values from 16 to 2048
- candidates: int32 [128, 64], P(('gx', 'gy')), may hold values from 0 to 131071, as said below
- item_table: bfloat16 [131072, 512], P(('gx', 'gy')), may hold values from -6 to 6
- value_weight: bfloat16 [256, 256], replicated, may hold values from -0.375 to 0.375
- click_hidden: bfloat16 [768, 256], replicated, may hold values from -0.21875 to 0.21875
- convert_hidden: bfloat16 [768, 256], replicated, may hold values from -0.21875 to 0.21875
- click_output: bfloat16 [256], replicated, may hold values from -0.75 to 0.75
- convert_output: bfloat16 [256], replicated, may hold values from -0.75 to 0.75
Outputs:
- click_rate: float32 [128, 64], P(('gx', 'gy'))
- click_conversion: float32 [128, 64], P(('gx', 'gy'))
The draws below stay inside these ranges and needn't reach their ends.
Inputs may be any that keep to these rules, and one draw needn't show every extreme that they name: Device k holds the table rows k * 4096 to (k + 1) * 4096 - 1. Of the 256 candidates of one device, at most 16 are items of one device's rows, and exactly 16 are items of some device's rows.
All inputs are finite; a program needn't handle non-finite values.
Results may differ from the reference program's by a relative error of at most 0.0028.
Values may be sent and summed in bfloat16 or wider, within the bound.
A program may use at most 64 MiB of HBM per device.

```python
import math
import jax
import jax.numpy as jnp
from jax import lax

D = 256
HEADS = 4
HEAD_DIM = 64
BLK = 128
MAXB = 16
U_DEV = 4
CAND = 64
ITEM_DEV = 4096
TH = 256
USERS = 128
ITEMS = 131072
CAP = 16
DEVICES = 32


def pick_candidates(key):
    impressions = U_DEV * CAND
    slot_total = DEVICES * CAP

    def per_device(device_key):
        key_order, key_full, key_shuffle, key_row = jax.random.split(device_key, 4)
        visit = jax.random.permutation(key_order, slot_total)
        ranking = jnp.zeros((slot_total,), jnp.int32).at[visit].set(jnp.arange(slot_total, dtype=jnp.int32))
        full_owner = jax.random.randint(key_full, (), 0, DEVICES)
        slot_owner = jnp.arange(slot_total, dtype=jnp.int32) // CAP
        priority = ranking - jnp.where(slot_owner == full_owner, slot_total, 0)
        chosen = jnp.argsort(priority)[:impressions].astype(jnp.int32)
        chosen = jax.random.permutation(key_shuffle, chosen)
        owner_device = chosen // CAP
        item_row = jax.random.randint(key_row, (impressions,), 0, ITEM_DEV)
        return (owner_device * ITEM_DEV + item_row).astype(jnp.int32)
    return jax.vmap(per_device)(jax.random.split(key, DEVICES)).reshape(USERS, CAND)


def make_table(key):
    return jax.random.truncated_normal(key, -6.0, 6.0, (ITEMS, 2 * D), jnp.float32)


def draw_candidates(key, part):
    return pick_candidates(jax.random.fold_in(key, 11))


def draw_item_table(key, part):
    return make_table(jax.random.fold_in(key, 12)).astype(jnp.bfloat16)


def draw_lengths(key, part):
    level_key, length_key = jax.random.split(jax.random.fold_in(key, 21))
    levels = jax.random.randint(level_key, (DEVICES, 1), 0, 4)
    highest = jnp.maximum(jnp.right_shift(jnp.full((DEVICES, 1), MAXB * BLK, jnp.int32), levels), BLK // 8 + 1)
    drawn = jax.random.randint(length_key, (DEVICES, U_DEV), BLK // 8, highest + 1)
    drawn = drawn.at[0, 0].set(MAXB * BLK).at[0, 1].set(BLK // 8)
    return drawn.reshape(USERS).astype(jnp.int32)


def draw_history(key, part):
    base_key = jax.random.fold_in(key, 13)
    return jax.random.truncated_normal(base_key, -6.0, 6.0, (USERS, MAXB * BLK, D), jnp.float32).astype(jnp.bfloat16)


def gaussian(own_key, extent, deviation, most, kind=jnp.bfloat16):
    values = jax.random.normal(own_key, extent, jnp.float32) * deviation
    return jnp.minimum(jnp.maximum(values, -most), most).astype(kind)


def setup_inputs(seed: int = 0) -> dict:
    seeds = jax.random.split(jax.random.key(seed), 10)
    return {
        "history": draw_history(jax.random.fold_in(seeds[9], 71), 0),
        "lengths": draw_lengths(jax.random.fold_in(seeds[9], 71), 0),
        "candidates": draw_candidates(jax.random.fold_in(seeds[9], 71), 0),
        "item_table": draw_item_table(jax.random.fold_in(seeds[9], 71), 0),
        "value_weight": gaussian(seeds[4], (D, D), D ** -0.5, 0.375),
        "click_hidden": gaussian(seeds[5], (3 * D, TH), (3 * D) ** -0.5, 0.21875),
        "convert_hidden": gaussian(seeds[6], (3 * D, TH), (3 * D) ** -0.5, 0.21875),
        "click_output": gaussian(seeds[7], (TH,), (TH // 4) ** -0.5, 0.75),
        "convert_output": gaussian(seeds[8], (TH,), (TH // 4) ** -0.5, 0.75),
    }


def reference(history, lengths, candidates, item_table, value_weight, click_hidden, convert_hidden, click_output, convert_output):
    scale_factor = 1.0 / math.sqrt(HEAD_DIM)
    candidate_rows = item_table[candidates]
    target = candidate_rows[:, :, :D]
    features = candidate_rows[:, :, D:]
    value_heads = value_weight.astype(jnp.float32).reshape(D, HEADS, HEAD_DIM)

    def one_user(user_args):
        user_history, user_length, user_target = user_args
        blocks = user_history.reshape(MAXB, BLK, D).astype(jnp.float32)
        block_heads = blocks.reshape(MAXB, BLK, HEADS, HEAD_DIM)
        query = user_target.astype(jnp.float32).reshape(CAND, HEADS, HEAD_DIM)
        scores = jnp.einsum('chj,bthj->bcht', query, block_heads) * scale_factor
        place = jnp.arange(MAXB, dtype=jnp.int32)[:, None] * BLK + jnp.arange(BLK, dtype=jnp.int32)[None, :]
        live_key = (place < user_length)[:, None, None, :]
        masked = jnp.where(live_key, scores, -1e+30)
        block_max = lax.optimization_barrier(jnp.max(masked, -1))
        weights = jnp.where(live_key, jnp.exp(masked - block_max[..., None]), 0.0).astype(jnp.bfloat16)
        block_sum = lax.optimization_barrier(jnp.sum(weights.astype(jnp.float32), -1))
        block_context = jnp.einsum('bcht,btd->bchd', weights.astype(jnp.float32), blocks)
        top_max = lax.optimization_barrier(jnp.max(block_max, 0))
        factor = jnp.exp(block_max - top_max)
        total = lax.optimization_barrier(jnp.sum(factor * block_sum, 0))
        context = lax.optimization_barrier(jnp.sum(factor[..., None] * block_context, 0))
        numerator = jnp.einsum('chd,dhk->chk', context, value_heads, precision=lax.Precision.HIGHEST)
        pooled = (numerator / total[..., None]).reshape(CAND, D)
        normed = pooled * lax.rsqrt(lax.optimization_barrier(jnp.mean(pooled * pooled, -1, keepdims=True)) + 1e-06)
        return normed.astype(jnp.bfloat16)
    interest = lax.map(one_user, (history, lengths, target))
    joined = jnp.concatenate([interest, target, features], -1).reshape(USERS * CAND, 3 * D)
    click_act = jax.nn.relu(jnp.dot(joined, click_hidden, preferred_element_type=jnp.float32)).astype(jnp.bfloat16)
    convert_act = jax.nn.relu(jnp.dot(joined, convert_hidden, preferred_element_type=jnp.float32)).astype(jnp.bfloat16)
    click_rate = jax.nn.sigmoid(jnp.dot(click_act, click_output, preferred_element_type=jnp.float32))
    convert_rate = jax.nn.sigmoid(jnp.dot(convert_act, convert_output, preferred_element_type=jnp.float32))
    return (click_rate.reshape(USERS, CAND), (click_rate * convert_rate).reshape(USERS, CAND))
```

```python
import functools
import math

import jax
import jax.numpy as jnp
from jax import lax
from jax.experimental import pallas as pl
from jax.experimental.pallas import tpu as pltpu
from jax.sharding import PartitionSpec as P

HEADS = 4
CHUNK = 512
SPLIT = 256
MESH = pl.DeviceIdType.MESH
neg_big = -1e30
f32, bf16 = jnp.float32, jnp.bfloat16


def dot(a, b, dims=((1,), (0,))):
    return lax.dot_general(a, b, (dims, ((), ())), preferred_element_type=f32)


def iota(shape, axis):
    return lax.broadcasted_iota(jnp.int32, shape, axis)


def exchange_kernel(
    n,
    ny,
    cap,
    cand_ref,
    table_hbm,
    out_ref,
    table,
    id_send,
    id_recv,
    slabs,
    rows_recv,
    sems,
):
    me = lax.axis_index("gx") * ny + lax.axis_index("gy")
    users, per_user = cand_ref.shape
    total = users * per_user
    table_rows = table.shape[0]

    load = pltpu.make_async_copy(table_hbm, table, sems.at[4])
    load.start()

    def at(j):
        d = lax.rem(me + j, n)
        return d, (lax.div(d, ny), lax.rem(d, ny))

    barrier = pltpu.get_barrier_semaphore()

    def greet(j, c):
        pl.semaphore_signal(barrier, inc=1, device_id=at(j)[1], device_id_type=MESH)
        return c

    lax.fori_loop(1, n, greet, 0)

    ids = jnp.concatenate([cand_ref[u : u + 1, :] for u in range(users)], axis=1)
    first = iota((n, total), 0) * table_rows
    local = ids - first
    mine = (local >= 0) & (local < table_rows)
    hot = jnp.where(mine, 1.0, 0.0).astype(f32)
    earlier = jnp.where(iota((total, total), 0) < iota((total, total), 1), 1.0, 0.0).astype(bf16)
    rank = jnp.sum(hot * dot(hot.astype(bf16), earlier), axis=0, keepdims=True)
    owner = jnp.sum(hot * iota((n, total), 0).astype(f32), axis=0, keepdims=True)
    slot = (owner * cap + rank).astype(jnp.int32)
    high = jnp.where(mine, local // SPLIT, 0).astype(f32).astype(bf16)
    low = jnp.where(mine, local % SPLIT, 0).astype(f32).astype(bf16)
    rank_i = rank.astype(jnp.int32)
    lane = iota((128, total), 0)
    at_high = jnp.where(lane == rank_i, 1.0, 0.0).astype(bf16)
    at_low = jnp.where(lane == rank_i + cap, 1.0, 0.0).astype(bf16)
    request = dot(high, at_high, ((1,), (1,))) + dot(low, at_low, ((1,), (1,)))
    for d in range(n):
        id_send[d] = request[d : d + 1, :]

    pl.semaphore_wait(barrier, n - 1)

    def ask(j, c):
        d, where = at(j)
        pltpu.make_async_remote_copy(
            src_ref=id_send.at[d],
            dst_ref=id_recv.at[me],
            send_sem=sems.at[0],
            recv_sem=sems.at[1],
            device_id=where,
            device_id_type=MESH,
        ).start()
        return c

    lax.fori_loop(1, n, ask, 0)
    id_recv[me] = id_send[me]

    same = iota((total, total), 0) == iota((total, total), 1)
    slot_col = jnp.sum(jnp.where(same, slot.astype(f32), 0.0), axis=1, keepdims=True)
    slot_col = slot_col.astype(jnp.int32)

    others = pl.ds(0, n - 1)

    def drain(ref, sem):
        pltpu.make_async_copy(ref.at[others], ref.at[others], sem).wait()

    load.wait()
    drain(id_recv, sems.at[1])

    group = 256 // cap
    asked = jnp.concatenate([id_recv[d] for d in range(n)], axis=0).astype(bf16)
    for g in range(n // group):
        base = g * group
        row = iota((256, n), 0)
        source = lax.rem(me + base + row // cap, n)
        expand = jnp.where(source == iota((256, n), 1), 1.0, 0.0).astype(bf16)
        spread = dot(expand, asked)
        place = iota((256, 128), 0) % cap
        lane = iota((256, 128), 1)
        weight = jnp.where(lane == place, float(SPLIT), jnp.where(lane == place + cap, 1.0, 0.0))
        wanted = jnp.sum(spread * weight, axis=1, keepdims=True).astype(jnp.int32)
        pick = jnp.where(wanted == iota((256, table_rows), 1), 1.0, 0.0).astype(bf16)
        found = dot(pick, table[...]).astype(bf16)
        for k in range(group):
            slabs[base + k] = found[k * cap : (k + 1) * cap, :]

        def answer(j, c):
            _, where = at(j)
            pltpu.make_async_remote_copy(
                src_ref=slabs.at[j],
                dst_ref=rows_recv.at[me],
                send_sem=sems.at[2],
                recv_sem=sems.at[3],
                device_id=where,
                device_id_type=MESH,
            ).start()
            return c

        lax.fori_loop(max(base, 1), base + group, answer, 0)
    rows_recv[me] = slabs[0]
    choose = jnp.where(slot_col == iota((total, n * cap), 1), 1.0, 0.0).astype(bf16)
    drain(rows_recv, sems.at[3])
    arrived = rows_recv[...].reshape(n * cap, rows_recv.shape[2])
    out_ref[...] = dot(choose, arrived).astype(bf16)
    drain(id_send, sems.at[0])
    drain(slabs, sems.at[2])


def exchange(candidates, item_table, n, ny):
    users, per_user = candidates.shape
    total = users * per_user
    table_rows, width = item_table.shape
    cap = max(2 * total // n, 16)
    return pl.pallas_call(
        functools.partial(exchange_kernel, n, ny, cap),
        out_shape=jax.ShapeDtypeStruct((total, width), bf16),
        in_specs=[
            pl.BlockSpec(memory_space=pltpu.VMEM),
            pl.BlockSpec(memory_space=pl.ANY),
        ],
        out_specs=pl.BlockSpec(memory_space=pltpu.VMEM),
        scratch_shapes=[
            pltpu.VMEM((table_rows, width), bf16),
            pltpu.VMEM((n, 1, 128), f32),
            pltpu.VMEM((n, 1, 128), f32),
            pltpu.VMEM((n, cap, width), bf16),
            pltpu.VMEM((n, cap, width), bf16),
            pltpu.SemaphoreType.DMA((5,)),
        ],
        compiler_params=pltpu.CompilerParams(collective_id=0, has_side_effects=True),
        name="exchange",
    )(candidates, item_table)


def attend_kernel(
    len_ref,
    hist_hbm,
    rows_ref,
    value_ref,
    click_ref,
    convert_ref,
    click_out_ref,
    convert_out_ref,
    rate_ref,
    both_ref,
    hist,
    joined,
    top_ref,
    sum_ref,
    ctx_ref,
    sems,
):
    users, seq, width = hist.shape
    per_user = rate_ref.shape[1]
    head = width // HEADS
    queries = HEADS * per_user
    chunks = seq // CHUNK
    scale = math.log2(math.e) / math.sqrt(head)

    def piece(u, c):
        rows = pl.ds(c * CHUNK, CHUNK)
        return pltpu.make_async_copy(hist_hbm.at[u, rows], hist.at[u, rows], sems.at[u, c])

    count = [(len_ref[u] + CHUNK - 1) // CHUNK for u in range(users)]
    for u in range(users):
        for c in range(chunks):

            @pl.when(c < count[u])
            def _():
                piece(u, c).start()

    lane_head = iota((per_user, width), 1) // head
    for u in range(users):
        mine = pl.ds(u * per_user, per_user)
        target = rows_ref[mine, :width]
        query = jnp.concatenate(
            [jnp.where(lane_head == h, target, jnp.zeros_like(target)) for h in range(HEADS)], axis=0
        )
        top_ref[...] = jnp.full(top_ref.shape, neg_big, f32)
        sum_ref[...] = jnp.zeros(sum_ref.shape, f32)
        ctx_ref[...] = jnp.zeros(ctx_ref.shape, f32)
        length = len_ref[u]

        def turn(c, carry):
            piece(u, c).wait()
            block = hist[u, pl.ds(pl.multiple_of(c * CHUNK, CHUNK), CHUNK), :]
            score = dot(query, block, ((1,), (1,))) * scale
            live = iota((queries, CHUNK), 1) < length - c * CHUNK
            score = jnp.where(live, score, neg_big)
            old = top_ref[...]
            new = jnp.maximum(old, jnp.max(score, axis=1, keepdims=True))
            weight = jnp.exp2(score - new).astype(bf16)
            keep = jnp.exp2(old - new)
            top_ref[...] = new
            sum_ref[...] = sum_ref[...] * keep + jnp.sum(weight.astype(f32), axis=1, keepdims=True)
            ctx_ref[...] = ctx_ref[...] * keep + dot(weight, block)
            return carry

        lax.fori_loop(0, count[u], turn, 0)
        context = ctx_ref[...]
        part0 = context.astype(bf16)
        rest = context - part0.astype(f32)
        part1 = rest.astype(bf16)
        part2 = (rest - part1.astype(f32)).astype(bf16)
        value = value_ref[...]
        full = (dot(part0, value) + dot(part1, value) + dot(part2, value)) / sum_ref[...]
        pooled = jnp.zeros((per_user, width), f32)
        for h in range(HEADS):
            pooled = jnp.where(lane_head == h, full[h * per_user : (h + 1) * per_user, :], pooled)
        normed = pooled * lax.rsqrt(jnp.mean(pooled * pooled, axis=1, keepdims=True) + 1e-6)
        joined[mine, :width] = normed.astype(bf16)
    joined[:, width:] = rows_ref[...]
    every = joined[...]

    def tower(hidden_ref, output_ref):
        act = jnp.maximum(dot(every, hidden_ref[...]), 0.0).astype(bf16)
        return 1.0 / (1.0 + jnp.exp(-dot(output_ref[...], act, ((1,), (1,)))))

    rate = tower(click_ref, click_out_ref)
    both = rate * tower(convert_ref, convert_out_ref)
    for u in range(users):
        mine = slice(u * per_user, (u + 1) * per_user)
        rate_ref[u : u + 1, :] = rate[:, mine]
        both_ref[u : u + 1, :] = both[:, mine]


def attend(history, lengths, rows, value, click, convert, click_out, convert_out, per_user):
    users, seq, width = history.shape
    queries = HEADS * per_user
    vmem = pl.BlockSpec(memory_space=pltpu.VMEM)
    out = jax.ShapeDtypeStruct((users, per_user), f32)
    return pl.pallas_call(
        attend_kernel,
        out_shape=(out, out),
        in_specs=[
            pl.BlockSpec(memory_space=pltpu.SMEM),
            pl.BlockSpec(memory_space=pl.ANY),
        ]
        + [vmem] * 6,
        out_specs=(vmem, vmem),
        scratch_shapes=[
            pltpu.VMEM((users, seq, width), bf16),
            pltpu.VMEM((users * per_user, 3 * width), bf16),
            pltpu.VMEM((queries, 1), f32),
            pltpu.VMEM((queries, 1), f32),
            pltpu.VMEM((queries, width), f32),
            pltpu.SemaphoreType.DMA((users, seq // CHUNK)),
        ],
        name="attend",
    )(lengths, history, rows, value, click, convert, click_out, convert_out)


def local(
    n,
    ny,
    history,
    lengths,
    candidates,
    item_table,
    value_weight,
    click_hidden,
    convert_hidden,
    click_output,
    convert_output,
):
    rows = exchange(candidates, item_table, n, ny)
    return attend(
        history,
        lengths,
        rows,
        value_weight,
        click_hidden,
        convert_hidden,
        click_output.reshape(1, -1),
        convert_output.reshape(1, -1),
        candidates.shape[1],
    )


def solution(mesh):
    both = ("gx", "gy")
    placed = (P(both, None, None), P(both), P(both, None), P(both, None), P(), P(), P(), P(), P())
    return jax.shard_map(
        functools.partial(local, mesh.shape["gx"] * mesh.shape["gy"], mesh.shape["gy"]),
        mesh=mesh,
        in_specs=placed,
        out_specs=(P(both, None), P(both, None)),
        check_vma=False,
    )
```

```python
import functools
import math

import jax
import jax.numpy as jnp
from jax import lax
from jax.experimental import pallas as pl
from jax.experimental.pallas import tpu as pltpu
from jax.sharding import PartitionSpec as P

HEADS = 4
CHUNK = 512
SPLIT = 256
MESH = pl.DeviceIdType.MESH
neg_big = -1e30
f32, bf16 = jnp.float32, jnp.bfloat16


def dot(a, b, dims=((1,), (0,))):
    return lax.dot_general(a, b, (dims, ((), ())), preferred_element_type=f32)


def iota(shape, axis):
    return lax.broadcasted_iota(jnp.int32, shape, axis)


def fused_kernel(
    n,
    ny,
    cap,
    len_ref,
    cand_ref,
    click_out_ref,
    convert_out_ref,
    table_hbm,
    hist_hbm,
    value_hbm,
    click_hbm,
    convert_hbm,
    rate_ref,
    both_ref,
    table,
    hist,
    value,
    click,
    convert,
    id_send,
    id_recv,
    pick,
    target_send,
    target_recv,
    feature_send,
    feature_recv,
    scores,
    tops,
    joined,
    load_sems,
    sems,
):
    me = lax.axis_index("gx") * ny + lax.axis_index("gy")
    users, per_user = cand_ref.shape
    seq, width = hist.shape[1:]
    total = users * per_user
    table_rows = table.shape[0]

    loads = [
        pltpu.make_async_copy(src, dst, load_sems.at[i])
        for i, (src, dst) in enumerate(
            [(table_hbm, table), (value_hbm, value), (click_hbm, click), (convert_hbm, convert)]
            + [(hist_hbm.at[u], hist.at[u]) for u in range(users)]
        )
    ]
    loads[0].start()

    def at(j):
        d = lax.rem(me + j, n)
        return d, (lax.div(d, ny), lax.rem(d, ny))

    barrier = pltpu.get_barrier_semaphore()

    def greet(j, c):
        pl.semaphore_signal(barrier, inc=1, device_id=at(j)[1], device_id_type=MESH)
        return c

    lax.fori_loop(1, n, greet, 0)
    for load in loads[4:] + loads[1:4]:
        load.start()

    ids = jnp.concatenate([cand_ref[u : u + 1, :] for u in range(users)], axis=1)
    first = iota((n, total), 0) * table_rows
    local = ids - first
    mine = (local >= 0) & (local < table_rows)
    hot = jnp.where(mine, 1.0, 0.0).astype(f32)
    earlier = jnp.where(iota((total, total), 0) < iota((total, total), 1), 1.0, 0.0).astype(bf16)
    rank = jnp.sum(hot * dot(hot.astype(bf16), earlier), axis=0, keepdims=True)
    owner = jnp.sum(hot * iota((n, total), 0).astype(f32), axis=0, keepdims=True)
    slot = owner * cap + rank
    high = jnp.where(mine, local // SPLIT, 0).astype(f32).astype(bf16)
    low = jnp.where(mine, local % SPLIT, 0).astype(f32).astype(bf16)
    rank_i = rank.astype(jnp.int32)
    lane = iota((128, total), 0)
    at_high = jnp.where(lane == rank_i, 1.0, 0.0).astype(bf16)
    at_low = jnp.where(lane == rank_i + cap, 1.0, 0.0).astype(bf16)
    request = dot(high, at_high, ((1,), (1,))) + dot(low, at_low, ((1,), (1,)))
    for d in range(n):
        id_send[d] = request[d : d + 1, :]

    def send(src, dst, lo, hi, sem, by_owner):
        def one(j, c):
            d, where = at(j)
            pltpu.make_async_remote_copy(
                src_ref=src.at[d if by_owner else j],
                dst_ref=dst.at[me],
                send_sem=sems.at[sem],
                recv_sem=sems.at[sem + 1],
                device_id=where,
                device_id_type=MESH,
            ).start()
            return c

        lax.fori_loop(max(lo, 1), hi, one, 0)

    others = pl.ds(0, n - 1)

    def drain(ref, sem):
        pltpu.make_async_copy(ref.at[others], ref.at[others], sems.at[sem]).wait()

    pl.semaphore_wait(barrier, n - 1)
    send(id_send, id_recv, 1, n, 0, True)
    id_recv[me] = id_send[me]

    same = iota((total, total), 0) == iota((total, total), 1)
    slot_col = jnp.sum(jnp.where(same, slot, 0.0), axis=1, keepdims=True).astype(jnp.int32)
    choose = jnp.where(slot_col == iota((total, n * cap), 1), 1.0, 0.0).astype(bf16)

    drain(id_recv, 1)
    group = 256 // cap
    asked = jnp.concatenate([id_recv[d] for d in range(n)], axis=0).astype(bf16)
    loads[0].wait()
    for g in range(n // group):
        base = g * group
        source = lax.rem(me + base + iota((256, n), 0) // cap, n)
        expand = jnp.where(source == iota((256, n), 1), 1.0, 0.0).astype(bf16)
        spread = dot(expand, asked)
        place = iota((256, 128), 0) % cap
        lane = iota((256, 128), 1)
        weight = jnp.where(lane == place, float(SPLIT), jnp.where(lane == place + cap, 1.0, 0.0))
        wanted = jnp.sum(spread * weight, axis=1, keepdims=True).astype(jnp.int32)
        pick[g] = jnp.where(wanted == iota((256, table_rows), 1), 1.0, 0.0).astype(bf16)
        found = dot(pick[g], table[:, :width]).astype(bf16)
        for k in range(group):
            target_send[base + k] = found[k * cap : (k + 1) * cap, :]
        send(target_send, target_recv, base, base + group, 2, False)
    for g in range(n // group):
        base = g * group
        found = dot(pick[g], table[:, width:]).astype(bf16)
        for k in range(group):
            feature_send[base + k] = found[k * cap : (k + 1) * cap, :]
        send(feature_send, feature_recv, base, base + group, 4, False)
    target_recv[me] = target_send[0]
    feature_recv[me] = feature_send[0]

    for load in loads[1:]:
        load.wait()
    drain(target_recv, 3)
    target = dot(choose, target_recv[...].reshape(n * cap, width)).astype(bf16)
    joined[:, width : 2 * width] = target

    head = width // HEADS
    queries = HEADS * per_user
    scale = math.log2(math.e) / math.sqrt(head)
    lane_head = iota((per_user, width), 1) // head
    chunks = seq // CHUNK
    slabs = CHUNK // 128

    def query_of(u):
        own = target[u * per_user : (u + 1) * per_user, :]
        return jnp.concatenate(
            [jnp.where(lane_head == h, own, jnp.zeros_like(own)) for h in range(HEADS)], axis=0
        )

    def score(u, c, query, top):
        s = dot(query, hist[u, c * CHUNK : (c + 1) * CHUNK, :], ((1,), (1,))) * scale
        live = iota((queries, CHUNK), 1) < len_ref[u] - c * CHUNK
        s = jnp.where(live, s, neg_big)
        scores[u % 2, :, c * CHUNK : (c + 1) * CHUNK] = s
        for k in range(slabs):
            part = s[:, k * 128 : (k + 1) * 128]
            top = part if top is None else jnp.maximum(top, part)
        return top

    def finish(u, top):
        tops[u % 2] = jnp.broadcast_to(jnp.max(top, axis=1, keepdims=True), (queries, 128))

    def gather(u, c, total_weight, context):
        top = tops[u % 2]
        parts = []
        for k in range(slabs):
            at_k = c * CHUNK + k * 128
            w = jnp.exp2(scores[u % 2, :, at_k : at_k + 128] - top).astype(bf16)
            wide = w.astype(f32)
            total_weight = wide if total_weight is None else total_weight + wide
            parts.append(w)
        more = dot(jnp.concatenate(parts, axis=1), hist[u, c * CHUNK : (c + 1) * CHUNK, :])
        return total_weight, more if context is None else context + more

    def interest(u, total_weight, context):
        part0 = context.astype(bf16)
        rest = context - part0.astype(f32)
        part1 = rest.astype(bf16)
        part2 = (rest - part1.astype(f32)).astype(bf16)
        full = dot(part0, value[...]) + dot(part1, value[...]) + dot(part2, value[...])
        full = full / jnp.sum(total_weight, axis=1, keepdims=True)
        pooled = jnp.zeros((per_user, width), f32)
        for h in range(HEADS):
            pooled = jnp.where(lane_head == h, full[h * per_user : (h + 1) * per_user, :], pooled)
        normed = pooled * lax.rsqrt(jnp.mean(pooled * pooled, axis=1, keepdims=True) + 1e-6)
        joined[u * per_user : (u + 1) * per_user, :width] = normed.astype(bf16)

    query = query_of(0)
    top = None
    for c in range(chunks):
        top = score(0, c, query, top)
    finish(0, top)
    for u in range(users):
        if u + 1 < users:
            query = query_of(u + 1)
        top = total_weight = context = None
        for c in range(chunks):
            if u + 1 < users:
                top = score(u + 1, c, query, top)
            total_weight, context = gather(u, c, total_weight, context)
        if u + 1 < users:
            finish(u + 1, top)
        interest(u, total_weight, context)

    drain(feature_recv, 5)
    feature = dot(choose, feature_recv[...].reshape(n * cap, width))
    joined[:, 2 * width :] = feature.astype(bf16)
    every = joined[...]

    def tower(hidden, output_ref):
        act = jnp.maximum(dot(every, hidden[...]), 0.0).astype(bf16)
        last = output_ref[...].reshape(1, -1)
        return 1.0 / (1.0 + jnp.exp(-dot(last, act, ((1,), (1,)))))

    rate = tower(click, click_out_ref)
    both = rate * tower(convert, convert_out_ref)
    for u in range(users):
        own = slice(u * per_user, (u + 1) * per_user)
        rate_ref[u : u + 1, :] = rate[:, own]
        both_ref[u : u + 1, :] = both[:, own]
    drain(id_send, 0)
    drain(target_send, 2)
    drain(feature_send, 4)


def local(
    n,
    ny,
    history,
    lengths,
    candidates,
    item_table,
    value_weight,
    click_hidden,
    convert_hidden,
    click_output,
    convert_output,
):
    users, per_user = candidates.shape
    seq, width = history.shape[1:]
    total = users * per_user
    cap = max(2 * total // n, 16)
    queries = HEADS * per_user
    vmem = pl.BlockSpec(memory_space=pltpu.VMEM)
    hbm = pl.BlockSpec(memory_space=pl.ANY)
    out = jax.ShapeDtypeStruct((users, per_user), f32)
    slab = pltpu.VMEM((n, cap, width), bf16)
    held = [item_table, history, value_weight, click_hidden, convert_hidden]
    return pl.pallas_call(
        functools.partial(fused_kernel, n, ny, cap),
        out_shape=(out, out),
        in_specs=[pl.BlockSpec(memory_space=pltpu.SMEM)] + [vmem] * 3 + [hbm] * 5,
        out_specs=(vmem, vmem),
        scratch_shapes=[pltpu.VMEM(x.shape, x.dtype) for x in held]
        + [
            pltpu.VMEM((n, 1, 128), f32),
            pltpu.VMEM((n, 1, 128), f32),
            pltpu.VMEM((n * cap // 256, 256, item_table.shape[0]), bf16),
            slab,
            slab,
            slab,
            slab,
            pltpu.VMEM((2, queries, seq), f32),
            pltpu.VMEM((2, queries, 128), f32),
            pltpu.VMEM((total, 3 * width), bf16),
            pltpu.SemaphoreType.DMA((4 + users,)),
            pltpu.SemaphoreType.DMA((6,)),
        ],
        compiler_params=pltpu.CompilerParams(collective_id=0, has_side_effects=True),
        name="esmm",
    )(lengths, candidates, click_output, convert_output, *held)


def solution(mesh):
    both = ("gx", "gy")
    placed = (P(both, None, None), P(both), P(both, None), P(both, None), P(), P(), P(), P(), P())
    return jax.shard_map(
        functools.partial(local, mesh.shape["gx"] * mesh.shape["gy"], mesh.shape["gy"]),
        mesh=mesh,
        in_specs=placed,
        out_specs=(P(both, None), P(both, None)),
        check_vma=False,
    )
```

```python
import functools
import math

import jax
import jax.numpy as jnp
from jax import lax
from jax.experimental import pallas as pl
from jax.experimental.pallas import tpu as pltpu
from jax.sharding import PartitionSpec as P

HEADS = 4
CHUNK = 512
SPLIT = 256
MESH = pl.DeviceIdType.MESH
neg_big = -1e30
f32, bf16 = jnp.float32, jnp.bfloat16


def dot(a, b, dims=((1,), (0,))):
    return lax.dot_general(a, b, (dims, ((), ())), preferred_element_type=f32)


def iota(shape, axis):
    return lax.broadcasted_iota(jnp.int32, shape, axis)


def fused_kernel(
    n,
    ny,
    cap,
    len_ref,
    cand_ref,
    click_out_ref,
    convert_out_ref,
    table_hbm,
    hist_hbm,
    value_hbm,
    click_hbm,
    convert_hbm,
    logit_ref,
    table,
    hist,
    value,
    click,
    convert,
    id_send,
    id_recv,
    pick,
    target_send,
    target_recv,
    feature_send,
    feature_recv,
    scores,
    tops,
    joined,
    load_sems,
    sems,
):
    me = lax.axis_index("gx") * ny + lax.axis_index("gy")
    users, per_user = cand_ref.shape
    seq, width = hist.shape[1:]
    total = users * per_user
    table_rows = table.shape[0]

    loads = [
        pltpu.make_async_copy(src, dst, load_sems.at[i])
        for i, (src, dst) in enumerate(
            [(table_hbm, table), (value_hbm, value), (click_hbm, click), (convert_hbm, convert)]
            + [(hist_hbm.at[u], hist.at[u]) for u in range(users)]
        )
    ]
    loads[0].start()

    half = n // ny // 2
    gx, gy = lax.axis_index("gx"), lax.axis_index("gy")
    upper = jnp.where(gx >= half, 1, 0)
    inner = gx - upper * half

    def walk(lo, hi, act):
        far = lo < n // 2
        skip = 0 if far else half
        start = (1 - upper if far else upper) * half

        def visit(a, b):
            x = inner + (a - skip)
            x = start + jnp.where(x >= half, x - half, x)
            y = gy + b
            y = jnp.where(y >= ny, y - ny, y)
            act(a * ny + b, x * ny + y, (x, y))

        def step(a, c):
            for b in range(ny):
                visit(a, b)
            return c

        first = lo // ny
        if lo == n // 2:
            for b in range(1, ny):
                visit(first, b)
            first += 1
        lax.fori_loop(first, hi // ny, step, 0)

    def greet(j, d, where):
        pl.semaphore_signal(barrier, inc=1, device_id=where, device_id_type=MESH)

    barrier = pltpu.get_barrier_semaphore()
    walk(0, n // 2, greet)
    walk(n // 2, n, greet)
    for load in loads[4:] + loads[1:4]:
        load.start()

    ids = jnp.concatenate([cand_ref[u : u + 1, :] for u in range(users)], axis=1)
    first = iota((n, total), 0) * table_rows
    local = ids - first
    mine = (local >= 0) & (local < table_rows)
    hot = jnp.where(mine, 1.0, 0.0).astype(f32)
    earlier = jnp.where(iota((total, total), 0) < iota((total, total), 1), 1.0, 0.0).astype(bf16)
    rank = jnp.sum(hot * dot(hot.astype(bf16), earlier), axis=0, keepdims=True)
    owner = jnp.sum(hot * iota((n, total), 0).astype(f32), axis=0, keepdims=True)
    slot = owner * cap + rank
    high = jnp.where(mine, local // SPLIT, 0).astype(f32).astype(bf16)
    low = jnp.where(mine, local % SPLIT, 0).astype(f32).astype(bf16)
    rank_i = rank.astype(jnp.int32)
    lane = iota((128, total), 0)
    at_high = jnp.where(lane == rank_i, 1.0, 0.0).astype(bf16)
    at_low = jnp.where(lane == rank_i + cap, 1.0, 0.0).astype(bf16)
    request = dot(high, at_high, ((1,), (1,))) + dot(low, at_low, ((1,), (1,)))
    for d in range(n):
        id_send[d] = request[d : d + 1, :]

    def send(src, dst, lo, hi, sem, by_owner):
        def one(j, d, where):
            pltpu.make_async_remote_copy(
                src_ref=src.at[d if by_owner else j],
                dst_ref=dst.at[me],
                send_sem=sems.at[sem],
                recv_sem=sems.at[sem + 1],
                device_id=where,
                device_id_type=MESH,
            ).start()

        walk(lo, hi, one)

    others = pl.ds(0, n - 1)

    def drain(ref, sem):
        pltpu.make_async_copy(ref.at[others], ref.at[others], sems.at[sem]).wait()

    pl.semaphore_wait(barrier, n - 1)
    send(id_send, id_recv, 0, n // 2, 0, True)
    send(id_send, id_recv, n // 2, n, 0, True)
    id_recv[me] = id_send[me]

    same = iota((total, total), 0) == iota((total, total), 1)
    slot_col = jnp.sum(jnp.where(same, slot, 0.0), axis=1, keepdims=True).astype(jnp.int32)
    choose = jnp.where(slot_col == iota((total, n * cap), 1), 1.0, 0.0).astype(bf16)

    drain(id_recv, 1)
    group = 256 // cap
    asked = jnp.concatenate([id_recv[d] for d in range(n)], axis=0).astype(bf16)
    loads[0].wait()
    for g in range(n // group):
        base = g * group
        order = base + iota((256, n), 0) // cap
        x = inner + order // ny
        if base >= n // 2:
            x = x - half
        x = jnp.where(x >= half, x - half, x)
        y = gy + order % ny
        source = ((1 - upper if base < n // 2 else upper) * half + x) * ny
        source = source + jnp.where(y >= ny, y - ny, y)
        expand = jnp.where(source == iota((256, n), 1), 1.0, 0.0).astype(bf16)
        spread = dot(expand, asked)
        place = iota((256, 128), 0) % cap
        lane = iota((256, 128), 1)
        weight = jnp.where(lane == place, float(SPLIT), jnp.where(lane == place + cap, 1.0, 0.0))
        wanted = jnp.sum(spread * weight, axis=1, keepdims=True).astype(jnp.int32)
        pick[g] = jnp.where(wanted == iota((256, table_rows), 1), 1.0, 0.0).astype(bf16)
        found = dot(pick[g], table[:, :width]).astype(bf16)
        for k in range(group):
            target_send[base + k] = found[k * cap : (k + 1) * cap, :]
        send(target_send, target_recv, base, base + group, 2, False)
    for g in range(n // group):
        base = g * group
        found = dot(pick[g], table[:, width:]).astype(bf16)
        for k in range(group):
            feature_send[base + k] = found[k * cap : (k + 1) * cap, :]
        send(feature_send, feature_recv, base, base + group, 4, False)
    target_recv[me] = target_send[n // 2]
    feature_recv[me] = feature_send[n // 2]

    for load in loads[1:]:
        load.wait()
    drain(target_recv, 3)
    target = dot(choose, target_recv[...].reshape(n * cap, width)).astype(bf16)
    joined[:, width : 2 * width] = target

    head = width // HEADS
    queries = HEADS * per_user
    scale = math.log2(math.e) / math.sqrt(head)
    lane_head = iota((per_user, width), 1) // head
    chunks = seq // CHUNK
    slabs = CHUNK // 128

    def query_of(u):
        own = target[u * per_user : (u + 1) * per_user, :]
        return jnp.concatenate(
            [jnp.where(lane_head == h, own, jnp.zeros_like(own)) for h in range(HEADS)], axis=0
        )

    def score(u, c, query, top):
        s = dot(query, hist[u, c * CHUNK : (c + 1) * CHUNK, :], ((1,), (1,))) * scale
        live = iota((queries, CHUNK), 1) < len_ref[u] - c * CHUNK
        s = jnp.where(live, s, neg_big)
        scores[u % 2, :, c * CHUNK : (c + 1) * CHUNK] = s
        for k in range(slabs):
            part = s[:, k * 128 : (k + 1) * 128]
            top = part if top is None else jnp.maximum(top, part)
        return top

    def finish(u, top):
        tops[u % 2] = jnp.broadcast_to(jnp.max(top, axis=1, keepdims=True), (queries, 128))

    def gather(u, c, total_weight, context):
        top = tops[u % 2]
        parts = []
        for k in range(slabs):
            at_k = c * CHUNK + k * 128
            w = jnp.exp2(scores[u % 2, :, at_k : at_k + 128] - top).astype(bf16)
            wide = w.astype(f32)
            total_weight = wide if total_weight is None else total_weight + wide
            parts.append(w)
        more = dot(jnp.concatenate(parts, axis=1), hist[u, c * CHUNK : (c + 1) * CHUNK, :])
        return total_weight, more if context is None else context + more

    def interest(u, total_weight, context):
        part0 = context.astype(bf16)
        rest = context - part0.astype(f32)
        part1 = rest.astype(bf16)
        part2 = (rest - part1.astype(f32)).astype(bf16)
        full = dot(part0, value[...]) + dot(part1, value[...]) + dot(part2, value[...])
        full = full / jnp.sum(total_weight, axis=1, keepdims=True)
        pooled = jnp.zeros((per_user, width), f32)
        for h in range(HEADS):
            pooled = jnp.where(lane_head == h, full[h * per_user : (h + 1) * per_user, :], pooled)
        normed = pooled * lax.rsqrt(jnp.mean(pooled * pooled, axis=1, keepdims=True) + 1e-6)
        joined[u * per_user : (u + 1) * per_user, :width] = normed.astype(bf16)

    query = query_of(0)
    top = None
    for c in range(chunks):
        top = score(0, c, query, top)
    finish(0, top)
    for u in range(users):
        if u + 1 < users:
            query = query_of(u + 1)
        top = total_weight = context = None
        for c in range(chunks):
            if u + 1 < users:
                top = score(u + 1, c, query, top)
            total_weight, context = gather(u, c, total_weight, context)
        if u + 1 < users:
            finish(u + 1, top)
        interest(u, total_weight, context)

    known = joined[...]
    early = [dot(known, hidden[: 2 * width, :]) for hidden in (click, convert)]
    drain(feature_recv, 5)
    feature = dot(choose, feature_recv[...].reshape(n * cap, width)).astype(bf16)
    for i, (hidden, output_ref) in enumerate([(click, click_out_ref), (convert, convert_out_ref)]):
        act = jnp.maximum(early[i] + dot(feature, hidden[2 * width :, :]), 0.0).astype(bf16)
        logit = dot(output_ref[...].reshape(1, -1), act, ((1,), (1,)))
        for u in range(users):
            logit_ref[i, u : u + 1, :] = logit[:, u * per_user : (u + 1) * per_user]
    drain(id_send, 0)
    drain(target_send, 2)
    drain(feature_send, 4)


def local(
    n,
    ny,
    history,
    lengths,
    candidates,
    item_table,
    value_weight,
    click_hidden,
    convert_hidden,
    click_output,
    convert_output,
):
    users, per_user = candidates.shape
    seq, width = history.shape[1:]
    total = users * per_user
    cap = max(2 * total // n, 16)
    queries = HEADS * per_user
    vmem = pl.BlockSpec(memory_space=pltpu.VMEM)
    hbm = pl.BlockSpec(memory_space=pl.ANY)
    out = jax.ShapeDtypeStruct((2, users, per_user), f32)
    slab = pltpu.VMEM((n, cap, width), bf16)
    held = [item_table, history, value_weight, click_hidden, convert_hidden]
    logits = pl.pallas_call(
        functools.partial(fused_kernel, n, ny, cap),
        out_shape=out,
        in_specs=[pl.BlockSpec(memory_space=pltpu.SMEM)] + [vmem] * 3 + [hbm] * 5,
        out_specs=vmem,
        scratch_shapes=[pltpu.VMEM(x.shape, x.dtype) for x in held]
        + [
            pltpu.VMEM((n, 1, 128), f32),
            pltpu.VMEM((n, 1, 128), f32),
            pltpu.VMEM((n * cap // 256, 256, item_table.shape[0]), bf16),
            slab,
            slab,
            slab,
            slab,
            pltpu.VMEM((2, queries, seq), f32),
            pltpu.VMEM((2, queries, 128), f32),
            pltpu.VMEM((total, 2 * width), bf16),
            pltpu.SemaphoreType.DMA((4 + users,)),
            pltpu.SemaphoreType.DMA((6,)),
        ],
        compiler_params=pltpu.CompilerParams(collective_id=0, has_side_effects=True),
        name="esmm",
    )(lengths, candidates, click_output, convert_output, *held)
    rate = jax.nn.sigmoid(logits[0])
    return rate, rate * jax.nn.sigmoid(logits[1])


def solution(mesh):
    both = ("gx", "gy")
    placed = (P(both, None, None), P(both), P(both, None), P(both, None), P(), P(), P(), P(), P())
    return jax.shard_map(
        functools.partial(local, mesh.shape["gx"] * mesh.shape["gy"], mesh.shape["gy"]),
        mesh=mesh,
        in_specs=placed,
        out_specs=(P(both, None), P(both, None)),
        check_vma=False,
    )
```
